512 devices in a mesh: dp: 8 (over x, core), feat: 64 (over z, y).
Axes of the slice: x: 4, y: 4, z: 16, core: 2. Of those that a mesh axis runs over, the one named last changes fastest.
Arguments:
- feature_slab: float32 [4096, 28672], P('dp', 'feat'), may hold values from -200 to 200, as said below
- basis_start: float32 [28672, 256], P('feat'), may hold values from -0.03125 to 0.03125
Outputs:
- basis_out: float32 [28672, 256], P('feat')
The draws below stay inside these ranges and needn't reach their ends.
Inputs may be any that keep to these rules, and one draw needn't show every extreme that they name: `feature_slab`: Real-valued entries; column scales differ over features and row scales over rows.
All inputs are finite; a program needn't handle non-finite values.
Results may differ from the reference program's by a relative error of at most 0.0015.
Values sent between devices are 32-bit elements; how exact they have to be, the bound alone decides.
No kernel may reach another device: no remote copies, remote signals or barrier semaphores. Data moves between devices by JAX's collectives and lax.ppermute only.
A program may use at most 64 MiB of HBM per device.

```python
import math
import jax
import jax.numpy as jnp
from jax import lax

FF = 28672
RANK = 256
ROWS = 512
ROUNDS = 1
NS_STEPS = 5
TOTAL_ROWS = 4096
N_DP = 8


def draw_feature_slab(key, part):
    key_cols, key_rows, key_vals = jax.random.split(jax.random.fold_in(key, 11), 3)
    column_scale = jnp.exp(jax.random.uniform(key_cols, (FF,), jnp.float32, 0.0, math.log(10.0)))
    column_scale = column_scale * jnp.exp(jnp.linspace(0.0, math.log(3.0), FF, dtype=jnp.float32))
    values = jax.random.normal(key_vals, (TOTAL_ROWS, FF), jnp.float32)
    row_scale = jnp.exp(jax.random.uniform(key_rows, (TOTAL_ROWS, 1), jnp.float32, 0.0, math.log(3.0)))
    return jnp.clip(values * row_scale * column_scale[None, :] / 8.0, -200.0, 200.0)


def steps_of(own_key, shape, cuts, least, high):
    factor_of = 1.0
    for dim, parts in cuts:
        heights = jax.random.uniform(jax.random.fold_in(jax.random.fold_in(own_key, 6), dim), (parts,), jnp.float32, least / len(cuts), high / len(cuts))
        factor_of = factor_of * jnp.repeat(jnp.exp(heights), shape[dim] // parts).reshape((-1,) + (1,) * (len(shape) - 1 - dim))
    return factor_of


def scatter_about(key, extent, deviation, reach, cuts=(), held_as=jnp.bfloat16):
    entries = jax.random.normal(key, extent, jnp.float32) * deviation
    if len(cuts) > 0:
        entries = steps_of(key, extent, cuts, -0.22, 0.18) * entries
    return jnp.clip(entries, min=-reach, max=reach).astype(held_as)


def setup_inputs(seed: int = 0) -> dict:
    key_of = jax.random.split(jax.random.key(seed), 3)
    feature_slab = draw_feature_slab(jax.random.fold_in(key_of[2], 71), 0)
    basis_start = scatter_about(key_of[1], (FF, RANK), FF ** -0.5, 0.03125, ((0, 64),), jnp.float32)
    return dict(feature_slab=feature_slab, basis_start=basis_start)


coef_first = 3.4445
coef_second = -4.775
coef_third = 2.0315

def plain_dot(left, right):
    return jnp.dot(left.astype(jnp.float32), right.astype(jnp.float32), precision=lax.Precision.HIGHEST, preferred_element_type=jnp.float32)

def newton_schulz(matrix):
    polar_iter = matrix / jnp.sqrt(jnp.sum(matrix * matrix) + 1e-12)
    for step_index in range(NS_STEPS):
        square_part = plain_dot(polar_iter, polar_iter.T)
        mixed_part = coef_second * square_part + coef_third * plain_dot(square_part, square_part)
        polar_iter = coef_first * polar_iter + plain_dot(mixed_part, polar_iter)
    return polar_iter

def group_round(group_slab, basis):
    projected = plain_dot(group_slab, basis)
    power_image = plain_dot(group_slab.T, projected)
    gram_matrix = plain_dot(power_image.T, power_image)
    lower_factor = jnp.linalg.cholesky(gram_matrix)
    identity = jnp.eye(RANK, dtype=basis.dtype)
    inverse = jax.scipy.linalg.solve_triangular(lower_factor, identity, lower=True)
    orthonormal = plain_dot(power_image, inverse.T)
    correlation = plain_dot(basis.T, orthonormal)
    return plain_dot(orthonormal, newton_schulz(correlation.T))

def reference(feature_slab, basis_start):
    basis = basis_start
    for round_index in range(ROUNDS):
        summed = jnp.zeros_like(basis)
        for group_index in range(N_DP):
            group_slab = feature_slab[group_index * ROWS:(group_index + 1) * ROWS]
            summed = summed + group_round(group_slab, basis)
        basis = summed / N_DP
    return basis * math.sqrt(FF)
```

```python
import math

import jax
import jax.numpy as jnp
from jax import lax
from jax.sharding import Mesh
from jax.sharding import PartitionSpec as P

FF = 28672
NS_STEPS = 5
FEAT = ("z_hi", "z_lo", "y")
PLANE = ("z_lo", "y")
DP = ("x", "core")

coef_first = 3.4445
coef_second = -4.775
coef_third = 2.0315


def summed_tiles(array, axis):
    peers = lax.axis_size(axis)
    tiles = array.reshape(peers, -1, *array.shape[1:])
    return jnp.sum(lax.all_to_all(tiles, axis, 0, 0, tiled=True), axis=0)


def from_everyone(array, axis):
    peers = lax.axis_size(axis)
    return lax.all_to_all(
        jnp.broadcast_to(array[None], (peers, *array.shape)), axis, 0, 0, tiled=True
    )


def copied_tiles(array, axis):
    everything = from_everyone(array, axis)
    return everything.reshape(-1, *array.shape[1:])


def summed_copies(array, axis):
    return jnp.sum(from_everyone(array, axis), axis=0)


def plain_dot(left, right):
    return jnp.dot(left, right, precision=lax.Precision.HIGHEST, preferred_element_type=jnp.float32)


def inner_dot(left, right):
    return lax.dot_general(
        left,
        right,
        (((0,), (0,)), ((), ())),
        precision=lax.Precision.HIGHEST,
        preferred_element_type=jnp.float32,
    )


def newton_schulz(matrix):
    polar_iter = matrix / jnp.sqrt(jnp.sum(matrix * matrix) + 1e-12)
    for step_index in range(NS_STEPS):
        square_part = plain_dot(polar_iter, polar_iter.T)
        mixed_part = coef_second * square_part + coef_third * plain_dot(square_part, square_part)
        polar_iter = coef_first * polar_iter + plain_dot(mixed_part, polar_iter)
    return polar_iter


def cholesky_inverse(gram_matrix):
    lower_factor = jnp.linalg.cholesky(gram_matrix)
    identity = jnp.eye(gram_matrix.shape[0], dtype=gram_matrix.dtype)
    return jax.scipy.linalg.solve_triangular(lower_factor, identity, lower=True)


def projected_sum(part):
    own = summed_tiles(summed_tiles(part, "y"), "z_lo")
    own = summed_copies(own, "z_hi")
    return copied_tiles(copied_tiles(own, "z_lo"), "y")


def gram_sum(power_image):
    half = power_image.shape[1] // 2
    left, right = power_image[:, :half], power_image[:, half:]
    part = jnp.concatenate([inner_dot(left, left), inner_dot(right, left), inner_dot(right, right)])
    own = summed_copies(summed_tiles(part, PLANE), "z_hi")
    top, cross, low = jnp.split(copied_tiles(own, PLANE), 3)
    return jnp.concatenate(
        [jnp.concatenate([top, cross.T], axis=1), jnp.concatenate([cross, low], axis=1)]
    )


def per_device(feature_slab, basis_start):
    groups = lax.axis_size(DP)
    projected = projected_sum(plain_dot(feature_slab, basis_start))
    power_image = inner_dot(feature_slab, projected)
    cross_terms = inner_dot(projected, projected)
    inverse = cholesky_inverse(gram_sum(power_image))
    correlation = plain_dot(cross_terms, inverse.T)
    aligned = plain_dot(power_image, plain_dot(inverse.T, newton_schulz(correlation.T)))
    own = summed_tiles(summed_tiles(aligned, "core"), "x") * (math.sqrt(FF) / groups)
    return copied_tiles(copied_tiles(own, "x"), "core")


def solution(mesh):
    torus = Mesh(mesh.devices.reshape(4, 2, 4, 4, 4), (*DP, *FEAT))
    return jax.shard_map(
        per_device,
        mesh=torus,
        in_specs=(P(DP, FEAT), P(FEAT, None)),
        out_specs=P(FEAT, None),
        check_vma=False,
    )
```
